16 devices in a mesh: ens: 2 (over y, z), sp: 8 (over x, core).
Axes of the slice: x: 4, y: 2, z: 1, core: 2. Of those that a mesh axis runs over, the one named last changes fastest.
The devices are a block of a 4x4x8 slice.
Arguments:
- x_seq: bfloat16 [16384, 512], P(('ens', 'sp')), parts along dimension 0
- w_past: bfloat16 [2, 8, 512, 512], replicated
- w_now: bfloat16 [2, 8, 512, 512], replicated
- b_conv: float32 [2, 8, 512], replicated
- w_res: bfloat16 [2, 8, 256, 512], replicated
- w_skip: bfloat16 [2, 8, 256, 256], replicated
- w_out1: bfloat16 [256, 256], replicated
- b_out1: float32 [256], replicated
- w_out2: bfloat16 [256, 256], replicated
- b_out2: float32 [256], replicated
Outputs:
- output 1: float32 [16384, 256], P(('ens', 'sp')), parts along dimension 0
- output 2: bfloat16 [16384, 512], P(('ens', 'sp')), parts along dimension 0
There are 2 independent parts. The reference program is written for one: setup_inputs(seed, part) draws one part's arguments, and reference() takes and returns one part's arrays. A program takes and returns all parts, laid end to end along the dimension named above; an argument that names none is the same for every part.
All inputs are finite; a program needn't handle non-finite values.
Results may differ from the reference program's by a relative error of at most 0.0140783.
Values are sent between devices in bfloat16 or wider.
A program may use at most 768 MiB of HBM per device.

```python
import jax
import jax.numpy as jnp
from jax import lax

SEQ_LEN = 8192
RES_CH = 512
GATE_CH = 256
SKIP_CH = 256
CLASSES = 256
DIL_CYCLE = 8
STACKS = 2
LAYERS_ALL = STACKS * DIL_CYCLE


def setup_inputs(seed: int = 0, part: int = 0) -> dict:
    root_key = jax.random.key(seed)
    subkeys = jax.random.split(root_key, 10)
    seq_key = jax.random.fold_in(subkeys[0], part)
    conv_shape = (STACKS, DIL_CYCLE, RES_CH, 2 * GATE_CH)
    conv_scale = (2 * RES_CH) ** -0.5
    proj_scale = 2.0 * (GATE_CH * LAYERS_ALL) ** -0.5
    head_scale = 2.0 * SKIP_CH ** -0.5
    x_seq = jax.random.normal(seq_key, (SEQ_LEN, RES_CH), jnp.float32)
    w_past = jax.random.normal(subkeys[1], conv_shape, jnp.float32) * conv_scale
    w_now = jax.random.normal(subkeys[2], conv_shape, jnp.float32) * conv_scale
    b_conv = jax.random.normal(subkeys[3], (STACKS, DIL_CYCLE, 2 * GATE_CH), jnp.float32) * 0.5
    w_res = jax.random.normal(subkeys[4], (STACKS, DIL_CYCLE, GATE_CH, RES_CH), jnp.float32) * proj_scale
    w_skip = jax.random.normal(subkeys[5], (STACKS, DIL_CYCLE, GATE_CH, SKIP_CH), jnp.float32) * proj_scale
    w_out1 = jax.random.normal(subkeys[6], (SKIP_CH, SKIP_CH), jnp.float32) * head_scale
    b_out1 = jax.random.normal(subkeys[7], (SKIP_CH,), jnp.float32) * 0.5
    w_out2 = jax.random.normal(subkeys[8], (SKIP_CH, CLASSES), jnp.float32) * head_scale
    b_out2 = jax.random.normal(subkeys[9], (CLASSES,), jnp.float32) * 0.5
    return {
        "x_seq": x_seq.astype(jnp.bfloat16),
        "w_past": w_past.astype(jnp.bfloat16),
        "w_now": w_now.astype(jnp.bfloat16),
        "b_conv": b_conv,
        "w_res": w_res.astype(jnp.bfloat16),
        "w_skip": w_skip.astype(jnp.bfloat16),
        "w_out1": w_out1.astype(jnp.bfloat16),
        "b_out1": b_out1,
        "w_out2": w_out2.astype(jnp.bfloat16),
        "b_out2": b_out2,
    }


def reference(x_seq, w_past, w_now, b_conv, w_res, w_skip, w_out1, b_out1, w_out2, b_out2):
    def stack_body(carry, stack_w):
        hidden, skip_sum = carry
        past_w, now_w, conv_b, res_w, skip_w = stack_w
        for layer_pos in range(DIL_CYCLE):
            dilation = 2 ** layer_pos
            shifted = jnp.concatenate([jnp.zeros((dilation, RES_CH), hidden.dtype), hidden[:SEQ_LEN - dilation]], axis=0)
            pre_act = (jnp.dot(shifted, past_w[layer_pos], preferred_element_type=jnp.float32)
                       + jnp.dot(hidden, now_w[layer_pos], preferred_element_type=jnp.float32)
                       + conv_b[layer_pos])
            gated = (jnp.tanh(pre_act[:, :GATE_CH]) * jax.nn.sigmoid(pre_act[:, GATE_CH:])).astype(jnp.bfloat16)
            hidden = (hidden.astype(jnp.float32) + jnp.dot(gated, res_w[layer_pos], preferred_element_type=jnp.float32)).astype(jnp.bfloat16)
            skip_sum = skip_sum + jnp.dot(gated, skip_w[layer_pos], preferred_element_type=jnp.float32)
        return (hidden, skip_sum), None

    skip_init = jnp.zeros((SEQ_LEN, SKIP_CH), jnp.float32)
    (hidden, skip_sum), _ = lax.scan(stack_body, (x_seq, skip_init), (w_past, w_now, b_conv, w_res, w_skip))
    skip_act = jax.nn.relu(skip_sum).astype(jnp.bfloat16)
    mid_act = jax.nn.relu(jnp.dot(skip_act, w_out1, preferred_element_type=jnp.float32) + b_out1).astype(jnp.bfloat16)
    logits = jnp.dot(mid_act, w_out2, preferred_element_type=jnp.float32) + b_out2
    return (logits, hidden)
```

```python
import functools

import jax
import jax.numpy as jnp
from jax import lax
from jax.experimental import pallas as pl
from jax.experimental.pallas import tpu as pltpu
from jax.sharding import PartitionSpec as P

TILE = 256
PAD = 128
MESH = pl.DeviceIdType.MESH


def order_of(layers, tiles, lag):
    keyed = []
    for layer in range(layers):
        for tile in range(tiles):
            back = tiles - 1 - tile
            keyed.append((tiles * layer + back * (1 + lag), layer, tile))
    return [(layer, tile) for _, layer, tile in sorted(keyed)]


def kernel(n, stacks, cycle, x_hbm, wp_hbm, wn_hbm, b_hbm, wr_hbm, ws_hbm, w1_hbm, c1_hbm, w2_hbm, c2_hbm,
           y_hbm, hout_hbm,
           h, skip, y, wz, wrs, b, w1, c1, w2, c2, halo,
           x_sem, w_sem, small_sem, send_sem, recv_sem, y_sem, h_sem):
    rows, res = x_hbm.shape
    gate = wr_hbm.shape[2]
    layers = stacks * cycle
    tiles = rows // TILE
    me = lax.axis_index("sp")
    right = lax.rem(me + 1, n)
    left = lax.rem(me + n - 1, n)
    ens = lax.axis_index("ens")

    barrier = pltpu.get_barrier_semaphore()
    pl.semaphore_signal(barrier, inc=1, device_id=(ens, left), device_id_type=MESH)

    def dilation(layer):
        return 2 ** (layer % cycle)

    def halo_rows(layer):
        return max(16, dilation(layer))

    x_copies = []
    for tile in range(tiles):
        x_copies.append(pltpu.make_async_copy(
            x_hbm.at[pl.ds(tile * TILE, TILE)], h.at[pl.ds(PAD + tile * TILE, TILE)], x_sem.at[tile]))
    w_copies = []
    for layer in range(layers):
        s, k = layer // cycle, layer % cycle
        w_copies.append([
            pltpu.make_async_copy(wp_hbm.at[s, k], wz.at[layer, pl.ds(0, res)], w_sem.at[layer]),
            pltpu.make_async_copy(wn_hbm.at[s, k], wz.at[layer, pl.ds(res, res)], w_sem.at[layer]),
            pltpu.make_async_copy(wr_hbm.at[s, k], wrs.at[layer, :, pl.ds(0, res)], w_sem.at[layer]),
            pltpu.make_async_copy(ws_hbm.at[s, k], wrs.at[layer, :, pl.ds(res, gate)], w_sem.at[layer]),
        ])
    small_copies = [
        pltpu.make_async_copy(b_hbm, b, small_sem.at[0]),
        pltpu.make_async_copy(w1_hbm, w1, small_sem.at[1]),
        pltpu.make_async_copy(c1_hbm, c1, small_sem.at[2]),
        pltpu.make_async_copy(w2_hbm, w2, small_sem.at[3]),
        pltpu.make_async_copy(c2_hbm, c2, small_sem.at[4]),
    ]
    x_copies[-1].start()
    small_copies[0].start()
    for c in w_copies[0]:
        c.start()
    for c in reversed(x_copies[:-1]):
        c.start()
    for layer in range(1, layers):
        for c in w_copies[layer]:
            c.start()
    for c in small_copies[1:]:
        c.start()

    def halo_send(layer):
        r = halo_rows(layer)
        return pltpu.make_async_remote_copy(
            src_ref=h.at[pl.ds(PAD + rows - r, r)],
            dst_ref=halo.at[layer, pl.ds(PAD - r, r)],
            send_sem=send_sem.at[layer], recv_sem=recv_sem.at[layer],
            device_id=(ens, right), device_id_type=MESH)

    def past_rows(tile, d):
        base = PAD + tile * TILE
        if d % 16 == 0:
            return h[pl.ds(base - d, TILE), :]
        wide = h[pl.ds(base - 16, TILE + 16), :].astype(jnp.float32)
        return wide[16 - d:16 - d + TILE].astype(jnp.bfloat16)

    pl.semaphore_wait(barrier, 1)

    x_ready, w_ready = set(), set()
    last_tile = tiles - 1

    def need_x(tile):
        if tile >= 0 and tile not in x_ready:
            x_ready.add(tile)
            x_copies[tile].wait()
            if tile == last_tile:
                halo_send(0).start()

    def need_w(layer):
        if layer not in w_ready:
            w_ready.add(layer)
            for c in w_copies[layer]:
                c.wait()

    small_ready = False
    for layer, tile in order_of(layers, tiles, 1):
        d = dilation(layer)
        if layer == 0:
            need_x(tile)
            need_x(tile - 1)
            if not small_ready:
                small_ready = True
                small_copies[0].wait()
        need_w(layer)
        if tile == 0:
            r = halo_rows(layer)
            halo_send(layer).wait_recv()
            got = halo[layer, pl.ds(PAD - r, r), :]
            h[pl.ds(PAD - r, r), :] = jnp.where(me > 0, got, jnp.zeros_like(got))
        mine = pl.ds(PAD + tile * TILE, TILE)
        now = h[mine, :]
        z = jnp.dot(jnp.concatenate([past_rows(tile, d), now], axis=1), wz[layer],
                    preferred_element_type=jnp.float32)
        s, k = layer // cycle, layer % cycle
        z = z + b[s, pl.ds(k, 1), :]
        g = (jnp.tanh(z[:, :gate]) * (0.5 * jnp.tanh(0.5 * z[:, gate:]) + 0.5)).astype(jnp.bfloat16)
        o = jnp.dot(g, wrs[layer], preferred_element_type=jnp.float32)
        if layer > 0 and tile == last_tile:
            halo_send(layer).wait_send()
        if layer == 0 and tile == last_tile:
            halo_send(0).wait_send()
        h[mine, :] = (now.astype(jnp.float32) + o[:, :res]).astype(jnp.bfloat16)
        rows_here = pl.ds(tile * TILE, TILE)
        if layer == 0:
            skip[rows_here, :] = o[:, res:]
        else:
            skip[rows_here, :] = skip[rows_here, :] + o[:, res:]
        if layer + 1 < layers and tile == last_tile:
            halo_send(layer + 1).start()
        if layer + 1 == layers:
            pltpu.make_async_copy(h.at[mine], hout_hbm.at[rows_here], h_sem.at[tile]).start()
            if tile == last_tile:
                for c in small_copies[1:]:
                    c.wait()
            a = jnp.maximum(skip[rows_here, :], 0.0).astype(jnp.bfloat16)
            m = jnp.dot(a, w1[...], preferred_element_type=jnp.float32) + c1[...]
            m = jnp.maximum(m, 0.0).astype(jnp.bfloat16)
            y[rows_here, :] = jnp.dot(m, w2[...], preferred_element_type=jnp.float32) + c2[...]
            pltpu.make_async_copy(y.at[rows_here], y_hbm.at[rows_here], y_sem.at[tile]).start()
    for tile in range(tiles):
        rows_here = pl.ds(tile * TILE, TILE)
        pltpu.make_async_copy(h.at[pl.ds(PAD + tile * TILE, TILE)], hout_hbm.at[rows_here], h_sem.at[tile]).wait()
        pltpu.make_async_copy(y.at[rows_here], y_hbm.at[rows_here], y_sem.at[tile]).wait()


def solution(mesh):
    n = mesh.shape["sp"]
    row_spec = P(("ens", "sp"), None)

    def local_stack(x_seq, w_past, w_now, b_conv, w_res, w_skip, w_out1, b_out1, w_out2, b_out2):
        stacks, cycle, res, _ = w_past.shape
        gate = b_conv.shape[-1] // 2
        skip_ch = w_skip.shape[-1]
        classes = w_out2.shape[-1]
        rows = x_seq.shape[0]
        layers = stacks * cycle
        tiles = rows // TILE
        any_spec = pl.BlockSpec(memory_space=pl.ANY)
        return pl.pallas_call(
            functools.partial(kernel, n, stacks, cycle),
            out_shape=(jax.ShapeDtypeStruct((rows, classes), jnp.float32),
                       jax.ShapeDtypeStruct((rows, res), jnp.bfloat16)),
            in_specs=[any_spec] * 10,
            out_specs=(any_spec, any_spec),
            scratch_shapes=[
                pltpu.VMEM((PAD + rows, res), jnp.bfloat16),
                pltpu.VMEM((rows, skip_ch), jnp.float32),
                pltpu.VMEM((rows, classes), jnp.float32),
                pltpu.VMEM((layers, 2 * res, 2 * gate), jnp.bfloat16),
                pltpu.VMEM((layers, gate, res + skip_ch), jnp.bfloat16),
                pltpu.VMEM(b_conv.shape, jnp.float32),
                pltpu.VMEM(w_out1.shape, jnp.bfloat16),
                pltpu.VMEM((1, skip_ch), jnp.float32),
                pltpu.VMEM(w_out2.shape, jnp.bfloat16),
                pltpu.VMEM((1, classes), jnp.float32),
                pltpu.VMEM((layers, PAD, res), jnp.bfloat16),
                pltpu.SemaphoreType.DMA((tiles,)),
                pltpu.SemaphoreType.DMA((layers,)),
                pltpu.SemaphoreType.DMA((5,)),
                pltpu.SemaphoreType.DMA((layers,)),
                pltpu.SemaphoreType.DMA((layers,)),
                pltpu.SemaphoreType.DMA((tiles,)),
                pltpu.SemaphoreType.DMA((tiles,)),
            ],
            compiler_params=pltpu.CompilerParams(
                collective_id=0, has_side_effects=True, vmem_limit_bytes=60 * 1024 * 1024),
            name="stack",
        )(x_seq, w_past, w_now, b_conv, w_res, w_skip, w_out1, b_out1.reshape(1, -1), w_out2, b_out2.reshape(1, -1))

    return jax.shard_map(
        local_stack,
        mesh=mesh,
        in_specs=(row_spec, P(), P(), P(), P(), P(), P(), P(), P(), P()),
        out_specs=(row_spec, row_spec),
        check_vma=False,
    )
```

```python
import functools

import jax
import jax.numpy as jnp
from jax import lax
from jax.experimental import pallas as pl
from jax.experimental.pallas import tpu as pltpu
from jax.sharding import PartitionSpec as P

TILE = 256
PIECE = 64
PAD = 128
SIDE = 256
BUFFERS = 4
LAGS = (5, 3, 2, 0)
MESH = pl.DeviceIdType.MESH
F32 = jnp.float32
BF16 = jnp.bfloat16


def program_of(layers, tiles, cycle):
    steps = sorted((tiles * layer + LAGS[tile], layer, tile) for layer in range(layers) for tile in range(tiles))
    items = [("z", layer, tile) for _, layer, tile in steps]
    hi, lo = (tiles - 1, tiles - 2), (tiles - 3, tiles - 4)
    half, end = cycle - 2, layers - 1
    at = items.index(("z", cycle - 2, 0))
    items.insert(at, ("s", lo, 0, half, False))
    items.insert(at - 1, ("s", hi, 0, half, False))
    at = items.index(("z", layers - 1, 0))
    items.insert(at, ("s", hi, half, end, False))
    items += [("s", hi, end, layers, True)]
    at = items.index(("z", layers - 1, 0))
    items.insert(at, ("s", lo, half, end, False))
    items += [("s", lo, end, layers, True)]
    return items


def group_bounds(layers, cycle):
    cuts = [0, 1, 3] + list(range(cycle, layers + 1, cycle))
    return list(zip(cuts[:-1], cuts[1:]))


def kernel(n, stacks, cycle, x_hbm, wp_hbm, wn_hbm, b_hbm, wr_hbm, ws_hbm, w1_hbm, c1_hbm, w2_hbm, c2_hbm,
           y, hout, h, skip, g_all, wz, wr, ws, b, w1, c1, w2, c2, halo, out_rows,
           x_sem, w_sem, small_sem, send_sem, recv_sem):
    rows, res = x_hbm.shape
    gate = wr_hbm.shape[2]
    layers = stacks * cycle
    tiles = rows // TILE
    me = lax.axis_index("sp")
    ens = lax.axis_index("ens")
    first, last = me == 0, me == n - 1

    barrier = pltpu.get_barrier_semaphore()

    @pl.when(jnp.logical_not(first))
    def _():
        pl.semaphore_signal(barrier, inc=1, device_id=(ens, me - 1), device_id_type=MESH)

    def where_of(layer):
        return layer // cycle, layer % cycle

    def dilation(layer):
        return 2 ** (layer % cycle)

    def halo_rows(layer):
        return max(16, dilation(layer))

    x_copies = [pltpu.make_async_copy(
        x_hbm.at[pl.ds(tile * TILE, TILE)], h.at[pl.ds(PAD + tile * TILE, TILE)], x_sem.at[tile])
        for tile in range(tiles)]
    groups = group_bounds(layers, cycle)
    group_of = {layer: i for i, (lo, hi) in enumerate(groups) for layer in range(lo, hi)}
    w_copies = []
    for i, (lo, hi) in enumerate(groups):
        s, k = where_of(lo)
        span = pl.ds(k, hi - lo)
        sem = w_sem.at[i]
        w_copies.append([
            pltpu.make_async_copy(wp_hbm.at[s, span], wz.at[pl.ds(lo, hi - lo), pl.ds(0, res)], sem),
            pltpu.make_async_copy(wn_hbm.at[s, span], wz.at[pl.ds(lo, hi - lo), pl.ds(res, res)], sem),
            pltpu.make_async_copy(wr_hbm.at[s, span], wr.at[pl.ds(lo, hi - lo)], sem),
            pltpu.make_async_copy(ws_hbm.at[s, span], ws.at[pl.ds(lo, hi - lo)], sem)])
    small_copies = [pltpu.make_async_copy(src, dst, small_sem.at[i]) for i, (src, dst) in enumerate(
        ((b_hbm, b), (w1_hbm, w1), (c1_hbm, c1), (w2_hbm, w2), (c2_hbm, c2)))]
    x_copies[-1].start()
    small_copies[0].start()
    for c in w_copies[0]:
        c.start()
    for c in reversed(x_copies[:-1]):
        c.start()
    for c in small_copies[1:]:
        c.start()

    def halo_send(layer, src):
        r = halo_rows(layer)
        return pltpu.make_async_remote_copy(
            src_ref=src, dst_ref=halo.at[layer, pl.ds(PAD - r, r)],
            send_sem=send_sem.at[layer], recv_sem=recv_sem.at[layer],
            device_id=(ens, lax.rem(me + 1, n)), device_id_type=MESH)

    def source(layer):
        r = halo_rows(layer)
        return out_rows.at[layer, pl.ds(PAD - r, r)]

    @pl.when(jnp.logical_not(last))
    def _():
        pl.semaphore_wait(barrier, 1)

    ready = set()

    def once(key, copies):
        if key not in ready:
            ready.add(key)
            for c in copies:
                c.wait()

    def start_send(layer):
        @pl.when(jnp.logical_not(last))
        def _():
            halo_send(layer, source(layer)).start()

    def keep_rows(layer):
        r = halo_rows(layer)
        out_rows[layer, pl.ds(PAD - r, r), :] = h[pl.ds(PAD + rows - r, r), :]

    def z_item(layer, tile):
        s, k = where_of(layer)
        d = dilation(layer)
        base = PAD + tile * TILE
        if layer == 0:
            for t in (tile, tile - 1):
                if t >= 0:
                    once(("x", t), [x_copies[t]])
            once("b", small_copies[:1])
            if tile == tiles - 1:
                keep_rows(0)
                start_send(0)
        group = group_of[layer]
        if ("w", group) not in ready:
            once(("w", group), w_copies[group])
            if group + 1 < len(groups):
                for c in w_copies[group + 1]:
                    c.start()
        if tile == 0:
            r = halo_rows(layer)

            @pl.when(jnp.logical_not(first))
            def _():
                halo_send(layer, source(layer)).wait_recv()
            got = halo[layer, pl.ds(PAD - r, r), :]
            h[pl.ds(PAD - r, r), :] = jnp.where(first, jnp.zeros_like(got), got)
        now = h[pl.ds(base, TILE), :]
        if d % 16 == 0:
            past = h[pl.ds(base - d, TILE), :]
        else:
            wide = h[pl.ds(base - 16, TILE + 16), :].astype(F32)
            past = wide[16 - d:16 - d + TILE].astype(BF16)
        z = jnp.dot(jnp.concatenate([past, now], axis=1), wz[layer], preferred_element_type=F32)
        t = jnp.tanh(z[:, :gate] + b[s, pl.ds(k, 1), pl.ds(0, gate)])
        u = jnp.tanh(z[:, gate:] * 0.5 + b[s, pl.ds(k, 1), pl.ds(gate, gate)] * 0.5)
        g = ((t * 0.5) * (u + 1.0)).astype(BF16)
        spot = pl.ds(tile * TILE, TILE)
        g_all[spot, pl.ds(layer * gate, gate)] = g
        new = (now.astype(F32) + jnp.dot(g, wr[layer], preferred_element_type=F32)).astype(BF16)
        if layer + 1 == layers:
            hout[spot, :] = new
        else:
            h[pl.ds(base, TILE), :] = new
        if layer + 1 < layers and tile == tiles - 1:
            keep_rows(layer + 1)
            start_send(layer + 1)

    started = set()

    def s_item(pair, begin, end, final):
        spot = pl.ds(min(pair) * TILE, 2 * TILE)
        v = jnp.dot(g_all[spot, pl.ds(begin * gate, (end - begin) * gate)],
                    ws[pl.ds(begin, end - begin)].reshape((end - begin) * gate, skip.shape[1]),
                    preferred_element_type=F32)
        if pair in started:
            v = skip[spot, :] + v
        started.add(pair)
        if not final:
            skip[spot, :] = v
            return
        once("head", small_copies[1:])
        a = jnp.maximum(v, 0.0).astype(BF16)
        m = jnp.maximum(jnp.dot(a, w1[...], preferred_element_type=F32) + c1[...], 0.0).astype(BF16)
        y[spot, :] = jnp.dot(m, w2[...], preferred_element_type=F32) + c2[...]

    for item in program_of(layers, tiles, cycle):
        if item[0] == "z":
            z_item(*item[1:])
        else:
            s_item(*item[1:])

    @pl.when(jnp.logical_not(last))
    def _():
        for layer in range(layers):
            halo_send(layer, source(layer)).wait_send()


def solution(mesh):
    n = mesh.shape["sp"]
    row_spec = P(("ens", "sp"), None)

    def local_stack(x_seq, w_past, w_now, b_conv, w_res, w_skip, w_out1, b_out1, w_out2, b_out2):
        stacks, cycle, res, _ = w_past.shape
        gate = b_conv.shape[-1] // 2
        skip_ch = w_skip.shape[-1]
        classes = w_out2.shape[-1]
        rows = x_seq.shape[0]
        layers = stacks * cycle
        tiles = rows // TILE
        args = (x_seq, w_past, w_now, b_conv, w_res, w_skip, w_out1, b_out1.reshape(1, -1), w_out2,
                b_out2.reshape(1, -1))
        args = [pltpu.with_memory_space_constraint(a, pltpu.HBM) for a in args]
        vmem = pl.BlockSpec(memory_space=pltpu.VMEM)
        return pl.pallas_call(
            functools.partial(kernel, n, stacks, cycle),
            out_shape=(jax.ShapeDtypeStruct((rows, classes), F32),
                       jax.ShapeDtypeStruct((rows, res), BF16)),
            in_specs=[pl.BlockSpec(memory_space=pl.ANY)] * 10,
            out_specs=(vmem, vmem),
            scratch_shapes=[
                pltpu.VMEM((PAD + rows, res), BF16),
                pltpu.VMEM((rows, skip_ch), F32),
                pltpu.VMEM((rows, layers * gate), BF16),
                pltpu.VMEM((layers, 2 * res, 2 * gate), BF16),
                pltpu.VMEM((layers,) + w_res.shape[2:], BF16),
                pltpu.VMEM((layers,) + w_skip.shape[2:], BF16),
                pltpu.VMEM(b_conv.shape, F32),
                pltpu.VMEM(w_out1.shape, BF16),
                pltpu.VMEM((1, skip_ch), F32),
                pltpu.VMEM(w_out2.shape, BF16),
                pltpu.VMEM((1, classes), F32),
                pltpu.VMEM((layers, PAD, res), BF16),
                pltpu.VMEM((layers, PAD, res), BF16),
                pltpu.SemaphoreType.DMA((tiles,)),
                pltpu.SemaphoreType.DMA((len(group_bounds(layers, cycle)),)),
                pltpu.SemaphoreType.DMA((5,)),
                pltpu.SemaphoreType.DMA((layers,)),
                pltpu.SemaphoreType.DMA((layers,)),
            ],
            compiler_params=pltpu.CompilerParams(
                collective_id=0, has_side_effects=True, vmem_limit_bytes=48 * 1024 * 1024),
            name="stack",
        )(*args)

    return jax.shard_map(
        local_stack,
        mesh=mesh,
        in_specs=(row_spec, P(), P(), P(), P(), P(), P(), P(), P(), P()),
        out_specs=(row_spec, row_spec),
        check_vma=False,
    )
```

```python
import functools

import jax
import jax.numpy as jnp
from jax import lax
from jax.experimental import pallas as pl
from jax.experimental.pallas import tpu as pltpu
from jax.sharding import PartitionSpec as P

TILE = 256
PAD = 128
JOINT = 5
LAGS = (5, 3, 2, 0)
MESH = pl.DeviceIdType.MESH
F32 = jnp.float32
BF16 = jnp.bfloat16


def program_of(layers, tiles, cycle):
    steps = sorted((tiles * layer + LAGS[tile], layer, tile) for layer in range(layers) for tile in range(tiles))
    items = [("z", layer, tile) for _, layer, tile in steps]
    hi, lo = (tiles - 1, tiles - 2), (tiles - 3, tiles - 4)
    half, end = cycle - 2, layers - 1
    at = items.index(("z", cycle - 2, 0))
    items[at:at] = [("s", hi, 0, half), ("s", lo, 0, half)]
    at = items.index(("z", layers - 1, 0))
    items[at:at] = [("s", hi, half, end), ("s", lo, half, end)]
    return items


def group_bounds(layers, cycle):
    cuts = [0, 1, 3, 5]
    while cuts[-1] < layers:
        cuts.append(min(cuts[-1] + (3 if cuts[-1] <= cycle else 5), layers))
    return list(zip(cuts[:-1], cuts[1:]))


def kernel(n, stacks, cycle, x_hbm, wp_hbm, wn_hbm, b_hbm, wr_hbm, ws_hbm, w1_hbm, c1_hbm, w2_hbm, c2_hbm,
           hout, skip, g_last, ws_last, w1, c1, w2, c2, h, g_all, wz, wr, ws, b, halo, out_rows,
           x_sem, w_sem, small_sem, send_sem, recv_sem):
    rows, res = x_hbm.shape
    gate = wr_hbm.shape[2]
    layers = stacks * cycle
    tiles = rows // TILE
    me = lax.axis_index("sp")
    ens = lax.axis_index("ens")
    first = me == 0
    joint = min(JOINT, cycle)

    barrier = pltpu.get_barrier_semaphore()

    pl.semaphore_signal(barrier, inc=1, device_id=(ens, lax.rem(me + n - 1, n)), device_id_type=MESH)

    def where_of(layer):
        return layer // cycle, layer % cycle

    def dilation(layer):
        return 2 ** (layer % cycle)

    def halo_rows(layer):
        k = layer % cycle
        if k == 0:
            return 2 ** joint
        return 0 if k < joint else dilation(layer)

    def extra_rows(layer):
        k = layer % cycle
        need = sum(2 ** j for j in range(k + 1, joint))
        return -(-need // 16) * 16

    x_copies = [pltpu.make_async_copy(
        x_hbm.at[pl.ds(tile * TILE, TILE)], h.at[pl.ds(PAD + tile * TILE, TILE)], x_sem.at[tile])
        for tile in range(tiles)]
    groups = group_bounds(layers, cycle)
    group_of = {layer: i for i, (lo, hi) in enumerate(groups) for layer in range(lo, hi)}
    w_copies = []
    for i, (lo, hi) in enumerate(groups):
        s, k = where_of(lo)
        span = pl.ds(k, hi - lo)
        sem = w_sem.at[i]
        w_copies.append([
            pltpu.make_async_copy(wp_hbm.at[s, span], wz.at[pl.ds(lo, hi - lo), pl.ds(0, res)], sem),
            pltpu.make_async_copy(wn_hbm.at[s, span], wz.at[pl.ds(lo, hi - lo), pl.ds(res, res)], sem),
            pltpu.make_async_copy(wr_hbm.at[s, span], wr.at[pl.ds(lo, hi - lo)], sem),
            pltpu.make_async_copy(ws_hbm.at[s, span], ws.at[pl.ds(lo, hi - lo)], sem)])
    small_copies = [pltpu.make_async_copy(src, dst, small_sem.at[i]) for i, (src, dst) in enumerate(
        ((b_hbm, b), (w1_hbm, w1), (c1_hbm, c1), (w2_hbm, w2), (c2_hbm, c2), (ws_hbm.at[stacks - 1, cycle - 1], ws_last)))]
    x_copies[-1].start()
    small_copies[0].start()
    for c in w_copies[0]:
        c.start()
    for c in reversed(x_copies[:-1]):
        c.start()
    for c in w_copies[1]:
        c.start(priority=1)

    def halo_send(layer, src):
        r = halo_rows(layer)
        return pltpu.make_async_remote_copy(
            src_ref=src, dst_ref=halo.at[layer, pl.ds(PAD - r, r)],
            send_sem=send_sem.at[layer], recv_sem=recv_sem.at[layer],
            device_id=(ens, lax.rem(me + 1, n)), device_id_type=MESH)

    def source(layer):
        r = halo_rows(layer)
        return out_rows.at[layer, pl.ds(PAD - r, r)]

    halo[layers, :, :] = jnp.zeros(halo.shape[1:], BF16)
    pl.semaphore_wait(barrier, 1)

    ready = set()

    def once(key, copies):
        if key not in ready:
            ready.add(key)
            for c in copies:
                c.wait()

    def start_send(layer):
        halo_send(layer, source(layer)).start()

    def keep_rows(layer):
        r = halo_rows(layer)
        out_rows[layer, pl.ds(PAD - r, r), :] = h[pl.ds(PAD + rows - r, r), :]

    def z_item(layer, tile):
        s, k = where_of(layer)
        d = dilation(layer)
        base = PAD + tile * TILE
        if layer == 0:
            for t in (tile, tile - 1):
                if t >= 0:
                    once(("x", t), [x_copies[t]])
            once("b", small_copies[:1])
            if tile == tiles - 1:
                keep_rows(0)
                start_send(0)
        group = group_of[layer]
        if ("w", group) not in ready:
            once(("w", group), w_copies[group])
            if 1 < group + 1 < len(groups):
                for c in w_copies[group + 1]:
                    c.start(priority=1)
            if group + 1 == len(groups):
                for c in small_copies[1:]:
                    c.start(priority=1)
        r = halo_rows(layer)
        if tile == 0 and r:
            @pl.when(jnp.logical_not(first))
            def _():
                halo_send(layer, source(layer)).wait_recv()
            slot = layer + (layers - layer) * ((n - me) // n)
            h[pl.ds(PAD - r, r), :] = halo[slot, pl.ds(PAD - r, r), :]
        extra = extra_rows(layer) if tile == 0 else 0
        start, size = base - extra, TILE + extra
        now = h[pl.ds(start, size), :]
        if d % 16 == 0:
            past = h[pl.ds(start - d, size), :]
        else:
            wide = h[pl.ds(start - 16, size + 16), :].astype(F32)
            past = wide[16 - d:16 - d + size].astype(BF16)
        z = jnp.dot(jnp.concatenate([past, now], axis=1), wz[layer], preferred_element_type=F32)
        t = jnp.tanh(z[:, :gate] + b[s, pl.ds(k, 1), pl.ds(0, gate)])
        u = jnp.tanh(z[:, gate:] * 0.5 + b[s, pl.ds(k, 1), pl.ds(gate, gate)] * 0.5)
        g = ((t * 0.5) * (u + 1.0)).astype(BF16)
        spot = pl.ds(tile * TILE, TILE)
        if layer + 1 == layers:
            g_last[spot, :] = g
        else:
            g_all[layer, spot, :] = g[extra:]
        new = (now.astype(F32) + jnp.dot(g, wr[layer], preferred_element_type=F32)).astype(BF16)
        if layer + 1 == layers:
            hout[spot, :] = new
        else:
            h[pl.ds(base, TILE), :] = new[extra:]
        if extra:
            h[pl.ds(start, extra), :] = jnp.where(first, jnp.zeros_like(new[:extra]), new[:extra])
        if layer + 1 < layers and tile == tiles - 1 and halo_rows(layer + 1):
            keep_rows(layer + 1)
            start_send(layer + 1)

    started = set()

    def s_item(pair, begin, end):
        spot = pl.ds(min(pair) * TILE, 2 * TILE)
        v = jnp.dot(jnp.concatenate([g_all[layer, spot, :] for layer in range(begin, end)], axis=1),
                    ws[pl.ds(begin, end - begin)].reshape((end - begin) * gate, skip.shape[1]),
                    preferred_element_type=F32)
        if pair in started:
            v = skip[spot, :] + v
        started.add(pair)
        skip[spot, :] = v

    for item in program_of(layers, tiles, cycle):
        if item[0] == "z":
            z_item(*item[1:])
        else:
            s_item(*item[1:])

    for c in small_copies[1:]:
        c.wait()
    exchanges = [layer for layer in range(layers) if halo_rows(layer)]
    for layer in exchanges:
        halo_send(layer, source(layer)).wait_send()

    @pl.when(first)
    def _():
        for layer in exchanges:
            halo_send(layer, source(layer)).wait_recv()


def head(h, skip, g, ws, w1, c1, w2, c2, y_hbm, hout_hbm, y, h_sem, y_sem):
    tiles = y.shape[0] // TILE
    h_copy = pltpu.make_async_copy(h, hout_hbm, h_sem)
    h_copy.start()
    copies = []
    for tile in range(tiles):
        spot = pl.ds(tile * TILE, TILE)
        v = skip[spot, :] + jnp.dot(g[spot, :], ws[...], preferred_element_type=F32)
        a = jnp.maximum(v, 0.0).astype(BF16)
        m = jnp.maximum(jnp.dot(a, w1[...], preferred_element_type=F32) + c1[...], 0.0).astype(BF16)
        y[spot, :] = jnp.dot(m, w2[...], preferred_element_type=F32) + c2[...]
        copies.append(pltpu.make_async_copy(y.at[spot], y_hbm.at[spot], y_sem.at[tile]))
        if tile % 2:
            for c in copies[-2:]:
                c.start()
    h_copy.wait()
    for c in copies:
        c.wait()


def solution(mesh):
    n = mesh.shape["sp"]
    row_spec = P(("ens", "sp"), None)

    def local_stack(x_seq, w_past, w_now, b_conv, w_res, w_skip, w_out1, b_out1, w_out2, b_out2):
        stacks, cycle, res, _ = w_past.shape
        gate = b_conv.shape[-1] // 2
        skip_ch = w_skip.shape[-1]
        classes = w_out2.shape[-1]
        rows = x_seq.shape[0]
        layers = stacks * cycle
        tiles = rows // TILE
        args = (x_seq, w_past, w_now, b_conv, w_res, w_skip, w_out1, b_out1.reshape(1, -1), w_out2,
                b_out2.reshape(1, -1))
        args = [pltpu.with_memory_space_constraint(a, pltpu.HBM) for a in args]
        vmem = pl.BlockSpec(memory_space=pltpu.VMEM)
        anywhere = pl.BlockSpec(memory_space=pl.ANY)
        parts = pl.pallas_call(
            functools.partial(kernel, n, stacks, cycle),
            out_shape=(jax.ShapeDtypeStruct((rows, res), BF16),
                       jax.ShapeDtypeStruct((rows, skip_ch), F32),
                       jax.ShapeDtypeStruct((rows, gate), BF16),
                       jax.ShapeDtypeStruct((gate, skip_ch), BF16),
                       jax.ShapeDtypeStruct(w_out1.shape, BF16),
                       jax.ShapeDtypeStruct((1, skip_ch), F32),
                       jax.ShapeDtypeStruct(w_out2.shape, BF16),
                       jax.ShapeDtypeStruct((1, classes), F32)),
            in_specs=[anywhere] * 10,
            out_specs=(vmem,) * 8,
            scratch_shapes=[
                pltpu.VMEM((PAD + rows, res), BF16),
                pltpu.VMEM((layers - 1, rows, gate), BF16),
                pltpu.VMEM((layers, 2 * res, 2 * gate), BF16),
                pltpu.VMEM((layers,) + w_res.shape[2:], BF16),
                pltpu.VMEM((layers,) + w_skip.shape[2:], BF16),
                pltpu.VMEM(b_conv.shape, F32),
                pltpu.VMEM((layers + 1, PAD, res), BF16),
                pltpu.VMEM((layers, PAD, res), BF16),
                pltpu.SemaphoreType.DMA((tiles,)),
                pltpu.SemaphoreType.DMA((len(group_bounds(layers, cycle)),)),
                pltpu.SemaphoreType.DMA((6,)),
                pltpu.SemaphoreType.DMA((layers,)),
                pltpu.SemaphoreType.DMA((layers,)),
            ],
            compiler_params=pltpu.CompilerParams(
                collective_id=0, has_side_effects=True, vmem_limit_bytes=48 * 1024 * 1024),
            name="stack",
        )(*args)
        return pl.pallas_call(
            head,
            out_shape=(jax.ShapeDtypeStruct((rows, classes), F32), jax.ShapeDtypeStruct((rows, res), BF16)),
            in_specs=[vmem] * 8,
            out_specs=(anywhere, anywhere),
            scratch_shapes=[pltpu.VMEM((rows, classes), F32), pltpu.SemaphoreType.DMA,
                            pltpu.SemaphoreType.DMA((tiles,))],
            compiler_params=pltpu.CompilerParams(vmem_limit_bytes=16 * 1024 * 1024),
            name="head",
        )(*parts)

    return jax.shard_map(
        local_stack,
        mesh=mesh,
        in_specs=(row_spec, P(), P(), P(), P(), P(), P(), P(), P(), P()),
        out_specs=(row_spec, row_spec),
        check_vma=False,
    )
```

```python
import functools

import jax
import jax.numpy as jnp
from jax import lax
from jax.experimental import pallas as pl
from jax.experimental.pallas import tpu as pltpu
from jax.sharding import PartitionSpec as P

TILE = 512
PAD = 128
JOINT = 5
LAGS = (1, 0)
MESH = pl.DeviceIdType.MESH
F32 = jnp.float32
BF16 = jnp.bfloat16


def program_of(layers, tiles, cycle):
    steps = sorted((tiles * layer + LAGS[tile], layer, tile) for layer in range(layers) for tile in range(tiles))
    items = [("z", layer, tile) for _, layer, tile in steps]
    hi = (1, 0)
    half, end = cycle - 2, layers - 1
    at = items.index(("z", cycle - 2, 0))
    items[at:at] = [("s", hi, 0, half)]
    at = items.index(("z", layers - 1, 0))
    items[at:at] = [("s", hi, half, end)]
    return items


def group_bounds(layers, cycle):
    cuts = [0, 1, 3, 5]
    while cuts[-1] < layers:
        cuts.append(min(cuts[-1] + (3 if cuts[-1] <= cycle else 5), layers))
    return list(zip(cuts[:-1], cuts[1:]))


def kernel(n, stacks, cycle, x_hbm, wp_hbm, wn_hbm, b_hbm, wr_hbm, ws_hbm, w1_hbm, c1_hbm, w2_hbm, c2_hbm,
           hout, skip, g_last, ws_last, w1, c1, w2, c2, h, g_all, wz, wr, ws, b, halo, out_rows,
           x_sem, w_sem, small_sem, send_sem, recv_sem):
    rows, res = x_hbm.shape
    gate = wr_hbm.shape[2]
    layers = stacks * cycle
    tiles = rows // TILE
    me = lax.axis_index("sp")
    ens = lax.axis_index("ens")
    first = me == 0
    joint = min(JOINT, cycle)

    barrier = pltpu.get_barrier_semaphore()

    pl.semaphore_signal(barrier, inc=1, device_id=(ens, lax.rem(me + n - 1, n)), device_id_type=MESH)

    def where_of(layer):
        return layer // cycle, layer % cycle

    def dilation(layer):
        return 2 ** (layer % cycle)

    def halo_rows(layer):
        k = layer % cycle
        if k == 0:
            return 2 ** joint
        return 0 if k < joint else dilation(layer)

    def extra_rows(layer):
        k = layer % cycle
        need = sum(2 ** j for j in range(k + 1, joint))
        return -(-need // 16) * 16

    x_copies = [pltpu.make_async_copy(
        x_hbm.at[pl.ds(tile * TILE, TILE)], h.at[pl.ds(PAD + tile * TILE, TILE)], x_sem.at[tile])
        for tile in range(tiles)]
    groups = group_bounds(layers, cycle)
    group_of = {layer: i for i, (lo, hi) in enumerate(groups) for layer in range(lo, hi)}
    w_copies = []
    for i, (lo, hi) in enumerate(groups):
        s, k = where_of(lo)
        span = pl.ds(k, hi - lo)
        sem = w_sem.at[i]
        w_copies.append([
            pltpu.make_async_copy(wp_hbm.at[s, span], wz.at[pl.ds(lo, hi - lo), pl.ds(0, res)], sem),
            pltpu.make_async_copy(wn_hbm.at[s, span], wz.at[pl.ds(lo, hi - lo), pl.ds(res, res)], sem),
            pltpu.make_async_copy(wr_hbm.at[s, span], wr.at[pl.ds(lo, hi - lo)], sem),
            pltpu.make_async_copy(ws_hbm.at[s, span], ws.at[pl.ds(lo, hi - lo)], sem)])
    small_copies = [pltpu.make_async_copy(src, dst, small_sem.at[i]) for i, (src, dst) in enumerate(
        ((b_hbm, b), (w1_hbm, w1), (c1_hbm, c1), (w2_hbm, w2), (c2_hbm, c2), (ws_hbm.at[stacks - 1, cycle - 1], ws_last)))]
    x_copies[-1].start()
    small_copies[0].start()
    for c in w_copies[0]:
        c.start()
    for c in reversed(x_copies[:-1]):
        c.start()
    for c in w_copies[1]:
        c.start(priority=1)

    def halo_send(layer, src):
        r = halo_rows(layer)
        return pltpu.make_async_remote_copy(
            src_ref=src, dst_ref=halo.at[layer, pl.ds(PAD - r, r)],
            send_sem=send_sem.at[layer], recv_sem=recv_sem.at[layer],
            device_id=(ens, lax.rem(me + 1, n)), device_id_type=MESH)

    def source(layer):
        r = halo_rows(layer)
        return out_rows.at[layer, pl.ds(PAD - r, r)]

    halo[layers, :, :] = jnp.zeros(halo.shape[1:], BF16)
    pl.semaphore_wait(barrier, 1)

    ready = set()

    def once(key, copies):
        if key not in ready:
            ready.add(key)
            for c in copies:
                c.wait()

    def start_send(layer):
        halo_send(layer, source(layer)).start()

    def keep_rows(layer):
        r = halo_rows(layer)
        out_rows[layer, pl.ds(PAD - r, r), :] = h[pl.ds(PAD + rows - r, r), :]

    def z_item(layer, tile):
        s, k = where_of(layer)
        d = dilation(layer)
        base = PAD + tile * TILE
        if layer == 0:
            for t in (tile, tile - 1):
                if t >= 0:
                    once(("x", t), [x_copies[t]])
            once("b", small_copies[:1])
            if tile == tiles - 1:
                keep_rows(0)
                start_send(0)
        group = group_of[layer]
        if ("w", group) not in ready:
            once(("w", group), w_copies[group])
            if 1 < group + 1 < len(groups):
                for c in w_copies[group + 1]:
                    c.start(priority=1)
            if group + 1 == len(groups):
                for c in small_copies[1:]:
                    c.start(priority=1)
        r = halo_rows(layer)
        if tile == 0 and r:
            @pl.when(jnp.logical_not(first))
            def _():
                halo_send(layer, source(layer)).wait_recv()
            slot = layer + (layers - layer) * ((n - me) // n)
            h[pl.ds(PAD - r, r), :] = halo[slot, pl.ds(PAD - r, r), :]
        extra = extra_rows(layer) if tile == 0 else 0
        start, size = base - extra, TILE + extra
        now = h[pl.ds(start, size), :]
        if d % 16 == 0:
            past = h[pl.ds(start - d, size), :]
        else:
            wide = h[pl.ds(start - 16, size + 16), :].astype(F32)
            past = wide[16 - d:16 - d + size].astype(BF16)
        z = (jnp.dot(past, wz[layer, pl.ds(0, res)], preferred_element_type=F32)
             + jnp.dot(now, wz[layer, pl.ds(res, res)], preferred_element_type=F32))
        t = jnp.tanh(z[:, :gate] + b[s, pl.ds(k, 1), pl.ds(0, gate)])
        u = jnp.tanh(z[:, gate:] * 0.5 + b[s, pl.ds(k, 1), pl.ds(gate, gate)] * 0.5)
        g = ((t * 0.5) * (u + 1.0)).astype(BF16)
        spot = pl.ds(tile * TILE, TILE)
        if layer + 1 == layers:
            g_last[spot, :] = g
        else:
            g_all[layer, spot, :] = g[extra:]
        new = (now.astype(F32) + jnp.dot(g, wr[layer], preferred_element_type=F32)).astype(BF16)
        if layer + 1 == layers:
            hout[spot, :] = new
        else:
            h[pl.ds(base, TILE), :] = new[extra:]
        if extra:
            h[pl.ds(start, extra), :] = jnp.where(first, jnp.zeros_like(new[:extra]), new[:extra])
        if layer + 1 < layers and tile == tiles - 1 and halo_rows(layer + 1):
            keep_rows(layer + 1)
            start_send(layer + 1)

    started = set()

    def s_item(pair, begin, end):
        spot = pl.ds(min(pair) * TILE, 2 * TILE)
        v = jnp.dot(jnp.concatenate([g_all[layer, spot, :] for layer in range(begin, end)], axis=1),
                    ws[pl.ds(begin, end - begin)].reshape((end - begin) * gate, skip.shape[1]),
                    preferred_element_type=F32)
        if pair in started:
            v = skip[spot, :] + v
        started.add(pair)
        skip[spot, :] = v

    for item in program_of(layers, tiles, cycle):
        if item[0] == "z":
            z_item(*item[1:])
        else:
            s_item(*item[1:])

    for c in small_copies[1:]:
        c.wait()
    exchanges = [layer for layer in range(layers) if halo_rows(layer)]
    for layer in exchanges:
        halo_send(layer, source(layer)).wait_send()

    @pl.when(first)
    def _():
        for layer in exchanges:
            halo_send(layer, source(layer)).wait_recv()


def head(h, skip, g, ws, w1, c1, w2, c2, y_hbm, hout_hbm, y, h_sem, y_sem):
    tiles = y.shape[0] // TILE
    h_copy = pltpu.make_async_copy(h, hout_hbm, h_sem)
    h_copy.start()
    copies = []
    for tile in range(tiles):
        spot = pl.ds(tile * TILE, TILE)
        v = skip[spot, :] + jnp.dot(g[spot, :], ws[...], preferred_element_type=F32)
        a = jnp.maximum(v, 0.0).astype(BF16)
        m = jnp.maximum(jnp.dot(a, w1[...], preferred_element_type=F32) + c1[...], 0.0).astype(BF16)
        y[spot, :] = jnp.dot(m, w2[...], preferred_element_type=F32) + c2[...]
        copies.append(pltpu.make_async_copy(y.at[spot], y_hbm.at[spot], y_sem.at[tile]))
        if tile % 2:
            for c in copies[-2:]:
                c.start()
    h_copy.wait()
    for c in copies:
        c.wait()


def solution(mesh):
    n = mesh.shape["sp"]
    row_spec = P(("ens", "sp"), None)

    def local_stack(x_seq, w_past, w_now, b_conv, w_res, w_skip, w_out1, b_out1, w_out2, b_out2):
        stacks, cycle, res, _ = w_past.shape
        gate = b_conv.shape[-1] // 2
        skip_ch = w_skip.shape[-1]
        classes = w_out2.shape[-1]
        rows = x_seq.shape[0]
        layers = stacks * cycle
        tiles = rows // TILE
        args = (x_seq, w_past, w_now, b_conv, w_res, w_skip, w_out1, b_out1.reshape(1, -1), w_out2,
                b_out2.reshape(1, -1))
        args = [pltpu.with_memory_space_constraint(a, pltpu.HBM) for a in args]
        vmem = pl.BlockSpec(memory_space=pltpu.VMEM)
        anywhere = pl.BlockSpec(memory_space=pl.ANY)
        parts = pl.pallas_call(
            functools.partial(kernel, n, stacks, cycle),
            out_shape=(jax.ShapeDtypeStruct((rows, res), BF16),
                       jax.ShapeDtypeStruct((rows, skip_ch), F32),
                       jax.ShapeDtypeStruct((rows, gate), BF16),
                       jax.ShapeDtypeStruct((gate, skip_ch), BF16),
                       jax.ShapeDtypeStruct(w_out1.shape, BF16),
                       jax.ShapeDtypeStruct((1, skip_ch), F32),
                       jax.ShapeDtypeStruct(w_out2.shape, BF16),
                       jax.ShapeDtypeStruct((1, classes), F32)),
            in_specs=[anywhere] * 10,
            out_specs=(vmem,) * 8,
            scratch_shapes=[
                pltpu.VMEM((PAD + rows, res), BF16),
                pltpu.VMEM((layers - 1, rows, gate), BF16),
                pltpu.VMEM((layers, 2 * res, 2 * gate), BF16),
                pltpu.VMEM((layers,) + w_res.shape[2:], BF16),
                pltpu.VMEM((layers,) + w_skip.shape[2:], BF16),
                pltpu.VMEM(b_conv.shape, F32),
                pltpu.VMEM((layers + 1, PAD, res), BF16),
                pltpu.VMEM((layers, PAD, res), BF16),
                pltpu.SemaphoreType.DMA((tiles,)),
                pltpu.SemaphoreType.DMA((len(group_bounds(layers, cycle)),)),
                pltpu.SemaphoreType.DMA((6,)),
                pltpu.SemaphoreType.DMA((layers,)),
                pltpu.SemaphoreType.DMA((layers,)),
            ],
            compiler_params=pltpu.CompilerParams(
                collective_id=0, has_side_effects=True, vmem_limit_bytes=48 * 1024 * 1024),
            name="stack",
        )(*args)
        return pl.pallas_call(
            head,
            out_shape=(jax.ShapeDtypeStruct((rows, classes), F32), jax.ShapeDtypeStruct((rows, res), BF16)),
            in_specs=[vmem] * 8,
            out_specs=(anywhere, anywhere),
            scratch_shapes=[pltpu.VMEM((rows, classes), F32), pltpu.SemaphoreType.DMA,
                            pltpu.SemaphoreType.DMA((tiles,))],
            compiler_params=pltpu.CompilerParams(vmem_limit_bytes=16 * 1024 * 1024),
            name="head",
        )(*parts)

    return jax.shard_map(
        local_stack,
        mesh=mesh,
        in_specs=(row_spec, P(), P(), P(), P(), P(), P(), P(), P(), P()),
        out_specs=(row_spec, row_spec),
        check_vma=False,
    )
```

```python
import functools

import jax
import jax.numpy as jnp
from jax import lax
from jax.experimental import pallas as pl
from jax.experimental.pallas import tpu as pltpu
from jax.sharding import PartitionSpec as P

TILE = 512
PAD = 128
JOINT = 5
LAGS = (1, 0)
MESH = pl.DeviceIdType.MESH
F32 = jnp.float32
BF16 = jnp.bfloat16


def program_of(layers, tiles, cycle):
    steps = sorted((tiles * layer + LAGS[tile], layer, tile) for layer in range(layers) for tile in range(tiles))
    items = [("z", layer, tile) for _, layer, tile in steps]
    hi = (1, 0)
    half, end = cycle - 2, layers - 1
    at = items.index(("z", cycle - 2, 0))
    items[at:at] = [("s", hi, 0, half)]
    at = items.index(("z", layers - 1, 0))
    items[at:at] = [("s", hi, half, end)]
    return items


def group_bounds(layers, cycle):
    cuts = [0, 1, 3, 5]
    while cuts[-1] < layers:
        cuts.append(min(cuts[-1] + (3 if cuts[-1] <= cycle else 5), layers))
    return list(zip(cuts[:-1], cuts[1:]))


def kernel(n, stacks, cycle, x_hbm, wp_hbm, wn_hbm, b_hbm, wr_hbm, ws_hbm, w1_hbm, c1_hbm, w2_hbm, c2_hbm,
           hout, skip, g_last, ws_last, w1, c1, w2, c2, h, g_all, wz, wr, ws, b, halo, out_rows,
           x_sem, w_sem, small_sem, send_sem, recv_sem):
    rows, res = x_hbm.shape
    gate = wr_hbm.shape[2]
    layers = stacks * cycle
    tiles = rows // TILE
    me = lax.axis_index("sp")
    ens = lax.axis_index("ens")
    first = me == 0
    joint = min(JOINT, cycle)

    barrier = pltpu.get_barrier_semaphore()

    pl.semaphore_signal(barrier, inc=1, device_id=(ens, lax.rem(me + n - 1, n)), device_id_type=MESH)

    def where_of(layer):
        return layer // cycle, layer % cycle

    def dilation(layer):
        return 2 ** (layer % cycle)

    def halo_rows(layer):
        k = layer % cycle
        if k == 0:
            return 2 ** joint
        return 0 if k < joint else dilation(layer)

    def extra_rows(layer):
        k = layer % cycle
        need = sum(2 ** j for j in range(k + 1, joint))
        return -(-need // 16) * 16

    x_copies = [pltpu.make_async_copy(
        x_hbm.at[pl.ds(tile * TILE, TILE)], h.at[pl.ds(PAD + tile * TILE, TILE)], x_sem.at[tile])
        for tile in range(tiles)]
    groups = group_bounds(layers, cycle)
    group_of = {layer: i for i, (lo, hi) in enumerate(groups) for layer in range(lo, hi)}
    w_copies = []
    for i, (lo, hi) in enumerate(groups):
        s, k = where_of(lo)
        span = pl.ds(k, hi - lo)
        sem = w_sem.at[i]
        w_copies.append([
            pltpu.make_async_copy(wp_hbm.at[s, span], wz.at[pl.ds(lo, hi - lo), pl.ds(0, res)], sem),
            pltpu.make_async_copy(wn_hbm.at[s, span], wz.at[pl.ds(lo, hi - lo), pl.ds(res, res)], sem),
            pltpu.make_async_copy(wr_hbm.at[s, span], wr.at[pl.ds(lo, hi - lo)], sem),
            pltpu.make_async_copy(ws_hbm.at[s, span], ws.at[pl.ds(lo, hi - lo)], sem)])
    small_copies = [pltpu.make_async_copy(src, dst, small_sem.at[i]) for i, (src, dst) in enumerate(
        ((b_hbm, b), (w1_hbm, w1), (c1_hbm, c1), (w2_hbm, w2), (c2_hbm, c2), (ws_hbm.at[stacks - 1, cycle - 1], ws_last)))]
    x_copies[-1].start()
    small_copies[0].start()
    for c in w_copies[0]:
        c.start()
    for c in reversed(x_copies[:-1]):
        c.start()
    for c in w_copies[1]:
        c.start(priority=1)

    def halo_send(layer, src):
        r = halo_rows(layer)
        return pltpu.make_async_remote_copy(
            src_ref=src, dst_ref=halo.at[layer, pl.ds(PAD - r, r)],
            send_sem=send_sem.at[layer], recv_sem=recv_sem.at[layer],
            device_id=(ens, lax.rem(me + 1, n)), device_id_type=MESH)

    def source(layer):
        r = halo_rows(layer)
        return out_rows.at[layer, pl.ds(PAD - r, r)]

    halo[layers, :, :] = jnp.zeros(halo.shape[1:], BF16)
    pl.semaphore_wait(barrier, 1)

    ready = set()

    def once(key, copies):
        if key not in ready:
            ready.add(key)
            for c in copies:
                c.wait()

    def start_send(layer):
        @pl.when(me < n - 1)
        def _():
            halo_send(layer, source(layer)).start()

    def keep_rows(layer):
        r = halo_rows(layer)
        out_rows[layer, pl.ds(PAD - r, r), :] = h[pl.ds(PAD + rows - r, r), :]

    def z_item(layer, tile):
        s, k = where_of(layer)
        d = dilation(layer)
        base = PAD + tile * TILE
        if layer == 0:
            for t in (tile, tile - 1):
                if t >= 0:
                    once(("x", t), [x_copies[t]])
            once("b", small_copies[:1])
            if tile == tiles - 1:
                keep_rows(0)
                start_send(0)
        group = group_of[layer]
        if ("w", group) not in ready:
            once(("w", group), w_copies[group])
            if 1 < group + 1 < len(groups):
                for c in w_copies[group + 1]:
                    c.start(priority=1)
            if group + 1 == len(groups):
                for c in small_copies[1:]:
                    c.start(priority=1)
        r = halo_rows(layer)
        if tile == 0 and r:
            @pl.when(jnp.logical_not(first))
            def _():
                halo_send(layer, source(layer)).wait_recv()
            slot = layer + (layers - layer) * ((n - me) // n)
            h[pl.ds(PAD - r, r), :] = halo[slot, pl.ds(PAD - r, r), :]
        extra = extra_rows(layer) if tile == 0 else 0
        start, size = base - extra, TILE + extra
        now = h[pl.ds(start, size), :]
        if d % 16 == 0:
            past = h[pl.ds(start - d, size), :]
        else:
            wide = h[pl.ds(start - 16, size + 16), :].astype(F32)
            past = wide[16 - d:16 - d + size].astype(BF16)
        z = (jnp.dot(past, wz[layer, pl.ds(0, res)], preferred_element_type=F32)
             + jnp.dot(now, wz[layer, pl.ds(res, res)], preferred_element_type=F32))
        t = jnp.tanh(z[:, :gate] + b[s, pl.ds(k, 1), pl.ds(0, gate)])
        u = jnp.tanh(z[:, gate:] * 0.5 + b[s, pl.ds(k, 1), pl.ds(gate, gate)] * 0.5)
        g = ((t * 0.5) * (u + 1.0)).astype(BF16)
        spot = pl.ds(tile * TILE, TILE)
        if layer + 1 == layers:
            g_last[spot, :] = g
        else:
            g_all[layer, spot, :] = g[extra:]
        new = (now.astype(F32) + jnp.dot(g, wr[layer], preferred_element_type=F32)).astype(BF16)
        if layer + 1 == layers:
            hout[spot, :] = new
        else:
            h[pl.ds(base, TILE), :] = new[extra:]
        if extra:
            h[pl.ds(start, extra), :] = jnp.where(first, jnp.zeros_like(new[:extra]), new[:extra])
        if layer + 1 < layers and tile == tiles - 1 and halo_rows(layer + 1):
            keep_rows(layer + 1)
            start_send(layer + 1)

    started = set()

    def s_item(pair, begin, end):
        weights = ws[pl.ds(begin, end - begin)].reshape((end - begin) * gate, skip.shape[1])
        for tile in pair:
            spot = pl.ds(tile * TILE, TILE)
            v = jnp.dot(jnp.concatenate([g_all[layer, spot, :] for layer in range(begin, end)], axis=1), weights,
                        preferred_element_type=F32)
            if pair in started:
                v = skip[spot, :] + v
            skip[spot, :] = v
        started.add(pair)

    for item in program_of(layers, tiles, cycle):
        if item[0] == "z":
            z_item(*item[1:])
        else:
            s_item(*item[1:])

    for c in small_copies[1:]:
        c.wait()
    exchanges = [layer for layer in range(layers) if halo_rows(layer)]

    @pl.when(me < n - 1)
    def _():
        for layer in exchanges:
            halo_send(layer, source(layer)).wait_send()


def head(h, skip, g, ws, w1, c1, w2, c2, y_hbm, hout_hbm, y, h_sem, y_sem):
    tiles = y.shape[0] // TILE
    h_copy = pltpu.make_async_copy(h, hout_hbm, h_sem)
    h_copy.start()
    copies = []
    for tile in range(tiles):
        spot = pl.ds(tile * TILE, TILE)
        v = skip[spot, :] + jnp.dot(g[spot, :], ws[...], preferred_element_type=F32)
        a = jnp.maximum(v, 0.0).astype(BF16)
        m = jnp.maximum(jnp.dot(a, w1[...], preferred_element_type=F32) + c1[...], 0.0).astype(BF16)
        y[spot, :] = jnp.dot(m, w2[...], preferred_element_type=F32) + c2[...]
        copies.append(pltpu.make_async_copy(y.at[spot], y_hbm.at[spot], y_sem.at[tile]))
        if tile % 2:
            for c in copies[-2:]:
                c.start()
    h_copy.wait()
    for c in copies:
        c.wait()


def solution(mesh):
    n = mesh.shape["sp"]
    row_spec = P(("ens", "sp"), None)

    def local_stack(x_seq, w_past, w_now, b_conv, w_res, w_skip, w_out1, b_out1, w_out2, b_out2):
        stacks, cycle, res, _ = w_past.shape
        gate = b_conv.shape[-1] // 2
        skip_ch = w_skip.shape[-1]
        classes = w_out2.shape[-1]
        rows = x_seq.shape[0]
        layers = stacks * cycle
        tiles = rows // TILE
        args = (x_seq, w_past, w_now, b_conv, w_res, w_skip, w_out1, b_out1.reshape(1, -1), w_out2,
                b_out2.reshape(1, -1))
        args = [pltpu.with_memory_space_constraint(a, pltpu.HBM) for a in args]
        vmem = pl.BlockSpec(memory_space=pltpu.VMEM)
        anywhere = pl.BlockSpec(memory_space=pl.ANY)
        parts = pl.pallas_call(
            functools.partial(kernel, n, stacks, cycle),
            out_shape=(jax.ShapeDtypeStruct((rows, res), BF16),
                       jax.ShapeDtypeStruct((rows, skip_ch), F32),
                       jax.ShapeDtypeStruct((rows, gate), BF16),
                       jax.ShapeDtypeStruct((gate, skip_ch), BF16),
                       jax.ShapeDtypeStruct(w_out1.shape, BF16),
                       jax.ShapeDtypeStruct((1, skip_ch), F32),
                       jax.ShapeDtypeStruct(w_out2.shape, BF16),
                       jax.ShapeDtypeStruct((1, classes), F32)),
            in_specs=[anywhere] * 10,
            out_specs=(vmem,) * 8,
            scratch_shapes=[
                pltpu.VMEM((PAD + rows, res), BF16),
                pltpu.VMEM((layers - 1, rows, gate), BF16),
                pltpu.VMEM((layers, 2 * res, 2 * gate), BF16),
                pltpu.VMEM((layers,) + w_res.shape[2:], BF16),
                pltpu.VMEM((layers,) + w_skip.shape[2:], BF16),
                pltpu.VMEM(b_conv.shape, F32),
                pltpu.VMEM((layers + 1, PAD, res), BF16),
                pltpu.VMEM((layers, PAD, res), BF16),
                pltpu.SemaphoreType.DMA((tiles,)),
                pltpu.SemaphoreType.DMA((len(group_bounds(layers, cycle)),)),
                pltpu.SemaphoreType.DMA((6,)),
                pltpu.SemaphoreType.DMA((layers,)),
                pltpu.SemaphoreType.DMA((layers,)),
            ],
            compiler_params=pltpu.CompilerParams(
                collective_id=0, has_side_effects=True, vmem_limit_bytes=48 * 1024 * 1024),
            name="stack",
        )(*args)
        return pl.pallas_call(
            head,
            out_shape=(jax.ShapeDtypeStruct((rows, classes), F32), jax.ShapeDtypeStruct((rows, res), BF16)),
            in_specs=[vmem] * 8,
            out_specs=(anywhere, anywhere),
            scratch_shapes=[pltpu.VMEM((rows, classes), F32), pltpu.SemaphoreType.DMA,
                            pltpu.SemaphoreType.DMA((tiles,))],
            compiler_params=pltpu.CompilerParams(vmem_limit_bytes=16 * 1024 * 1024),
            name="head",
        )(*parts)

    return jax.shard_map(
        local_stack,
        mesh=mesh,
        in_specs=(row_spec, P(), P(), P(), P(), P(), P(), P(), P(), P()),
        out_specs=(row_spec, row_spec),
        check_vma=False,
    )
```

```python
import functools

import jax
import jax.numpy as jnp
from jax import lax
from jax.experimental import pallas as pl
from jax.experimental.pallas import tpu as pltpu
from jax.sharding import PartitionSpec as P

TILE = 512
PAD = 128
JOINT = 5
LAGS = (1, 0)
MESH = pl.DeviceIdType.MESH
F32 = jnp.float32
BF16 = jnp.bfloat16


def program_of(layers, tiles, cycle):
    steps = sorted((tiles * layer + LAGS[tile], layer, tile) for layer in range(layers) for tile in range(tiles))
    items = [("z", layer, tile) for _, layer, tile in steps]
    hi = (1, 0)
    half, end = cycle - 2, layers - 1
    at = items.index(("z", cycle - 2, 0))
    items[at:at] = [("s", hi, 0, half)]
    at = items.index(("z", layers - 1, 0))
    items[at:at] = [("s", hi, half, end)]
    return items


def group_bounds(layers, cycle):
    cuts = [0, 1, 3, 5]
    while cuts[-1] < layers:
        cuts.append(min(cuts[-1] + (3 if cuts[-1] <= cycle else 5), layers))
    return list(zip(cuts[:-1], cuts[1:]))


def kernel(n, stacks, cycle, x_hbm, wp_hbm, wn_hbm, b_hbm, wr_hbm, ws_hbm, w1_hbm, c1_hbm, w2_hbm, c2_hbm,
           hout, skip, g_last, ws_last, w1, c1, w2, c2, h, g_all, wz, wr, ws, b, halo, out_rows,
           x_sem, w_sem, small_sem, send_sem, recv_sem):
    rows, res = x_hbm.shape
    gate = wr_hbm.shape[2]
    layers = stacks * cycle
    tiles = rows // TILE
    me = lax.axis_index("sp")
    ens = lax.axis_index("ens")
    first = me == 0
    joint = min(JOINT, cycle)

    barrier = pltpu.get_barrier_semaphore()

    pl.semaphore_signal(barrier, inc=1, device_id=(ens, lax.rem(me + n - 1, n)), device_id_type=MESH)

    def where_of(layer):
        return layer // cycle, layer % cycle

    def dilation(layer):
        return 2 ** (layer % cycle)

    def halo_rows(layer):
        k = layer % cycle
        if k == 0:
            return 2 ** joint
        return 0 if k < joint else dilation(layer)

    def extra_rows(layer):
        k = layer % cycle
        need = sum(2 ** j for j in range(k + 1, joint))
        return -(-need // 16) * 16

    x_copies = [pltpu.make_async_copy(
        x_hbm.at[pl.ds(tile * TILE, TILE)], h.at[pl.ds(PAD + tile * TILE, TILE)], x_sem.at[tile])
        for tile in range(tiles)]
    groups = group_bounds(layers, cycle)
    group_of = {layer: i for i, (lo, hi) in enumerate(groups) for layer in range(lo, hi)}
    w_copies = []
    for i, (lo, hi) in enumerate(groups):
        s, k = where_of(lo)
        span = pl.ds(k, hi - lo)
        sem = w_sem.at[i]
        w_copies.append([
            pltpu.make_async_copy(wp_hbm.at[s, span], wz.at[pl.ds(lo, hi - lo), pl.ds(0, res)], sem),
            pltpu.make_async_copy(wn_hbm.at[s, span], wz.at[pl.ds(lo, hi - lo), pl.ds(res, res)], sem),
            pltpu.make_async_copy(wr_hbm.at[s, span], wr.at[pl.ds(lo, hi - lo)], sem),
            pltpu.make_async_copy(ws_hbm.at[s, span], ws.at[pl.ds(lo, hi - lo)], sem)])
    small_copies = [pltpu.make_async_copy(src, dst, small_sem.at[i]) for i, (src, dst) in enumerate(
        ((b_hbm, b), (w1_hbm, w1), (c1_hbm, c1), (w2_hbm, w2), (c2_hbm, c2), (ws_hbm.at[stacks - 1, cycle - 1], ws_last)))]
    x_copies[-1].start()
    small_copies[0].start()
    for c in w_copies[0]:
        c.start()
    for c in reversed(x_copies[:-1]):
        c.start()
    for c in w_copies[1]:
        c.start(priority=1)

    def halo_send(layer, src):
        r = halo_rows(layer)
        return pltpu.make_async_remote_copy(
            src_ref=src, dst_ref=halo.at[layer, pl.ds(PAD - r, r)],
            send_sem=send_sem.at[layer], recv_sem=recv_sem.at[layer],
            device_id=(ens, lax.rem(me + 1, n)), device_id_type=MESH)

    def source(layer):
        r = halo_rows(layer)
        return out_rows.at[layer, pl.ds(PAD - r, r)]

    halo[layers, :, :] = jnp.zeros(halo.shape[1:], BF16)
    pl.semaphore_wait(barrier, 1)

    ready = set()

    def once(key, copies):
        if key not in ready:
            ready.add(key)
            for c in copies:
                c.wait()

    def start_send(layer):
        @pl.when(me < n - 1)
        def _():
            halo_send(layer, source(layer)).start()

    def keep_rows(layer):
        r = halo_rows(layer)
        out_rows[layer, pl.ds(PAD - r, r), :] = h[pl.ds(PAD + rows - r, r), :]

    def z_item(layer, tile):
        s, k = where_of(layer)
        d = dilation(layer)
        base = PAD + tile * TILE
        if layer == 0:
            for t in (tile, tile - 1):
                if t >= 0:
                    once(("x", t), [x_copies[t]])
            once("b", small_copies[:1])
            if tile == tiles - 1:
                keep_rows(0)
                start_send(0)
        group = group_of[layer]
        if ("w", group) not in ready:
            once(("w", group), w_copies[group])
            if 1 < group + 1 < len(groups):
                for c in w_copies[group + 1]:
                    c.start(priority=1)
            if group + 1 == len(groups):
                for c in small_copies[1:]:
                    c.start(priority=1)
        r = halo_rows(layer)
        if tile == 0 and r:
            @pl.when(jnp.logical_not(first))
            def _():
                halo_send(layer, source(layer)).wait_recv()
            slot = layer + (layers - layer) * ((n - me) // n)
            h[pl.ds(PAD - r, r), :] = halo[slot, pl.ds(PAD - r, r), :]
        extra = extra_rows(layer) if tile == 0 else 0
        start, size = base - extra, TILE + extra
        now = h[pl.ds(start, size), :]
        if d % 16 == 0:
            past = h[pl.ds(start - d, size), :]
        else:
            wide = h[pl.ds(start - 16, size + 16), :].astype(F32)
            past = wide[16 - d:16 - d + size].astype(BF16)
        z = (jnp.dot(past, wz[layer, pl.ds(0, res)], preferred_element_type=F32)
             + jnp.dot(now, wz[layer, pl.ds(res, res)], preferred_element_type=F32))
        t = jnp.tanh(z[:, :gate] + b[s, pl.ds(k, 1), pl.ds(0, gate)])
        u = jnp.tanh(z[:, gate:] * 0.5 + b[s, pl.ds(k, 1), pl.ds(gate, gate)] * 0.5)
        g = ((t * 0.5) * (u + 1.0)).astype(BF16)
        spot = pl.ds(tile * TILE, TILE)
        if layer + 1 == layers:
            g_last[spot, :] = g
        else:
            g_all[layer, spot, :] = g[extra:]
        cut = size - TILE // 2
        new = jnp.concatenate([
            (now[lo:hi].astype(F32) + jnp.dot(g[lo:hi], wr[layer], preferred_element_type=F32)).astype(BF16)
            for lo, hi in ((0, cut), (cut, size))], axis=0)
        if layer + 1 == layers:
            hout[spot, :] = new
        else:
            h[pl.ds(base, TILE), :] = new[extra:]
        if extra:
            h[pl.ds(start, extra), :] = jnp.where(first, jnp.zeros_like(new[:extra]), new[:extra])
        if layer + 1 < layers and tile == tiles - 1 and halo_rows(layer + 1):
            keep_rows(layer + 1)
            start_send(layer + 1)

    started = set()

    def s_item(pair, begin, end):
        weights = ws[pl.ds(begin, end - begin)].reshape((end - begin) * gate, skip.shape[1])
        for part in range(2 * len(pair)):
            spot = pl.ds(part * (TILE // 2), TILE // 2)
            v = jnp.dot(jnp.concatenate([g_all[layer, spot, :] for layer in range(begin, end)], axis=1), weights,
                        preferred_element_type=F32)
            if pair in started:
                v = skip[spot, :] + v
            skip[spot, :] = v
        started.add(pair)

    for item in program_of(layers, tiles, cycle):
        if item[0] == "z":
            z_item(*item[1:])
        else:
            s_item(*item[1:])

    for c in small_copies[1:]:
        c.wait()
    exchanges = [layer for layer in range(layers) if halo_rows(layer)]

    @pl.when(me < n - 1)
    def _():
        for layer in exchanges:
            halo_send(layer, source(layer)).wait_send()


def head(h, skip, g, ws, w1, c1, w2, c2, y_hbm, hout_hbm, y, h_sem, y_sem):
    tiles = y.shape[0] // TILE
    h_copy = pltpu.make_async_copy(h, hout_hbm, h_sem)
    h_copy.start()
    copies = []
    for tile in range(tiles):
        spot = pl.ds(tile * TILE, TILE)
        v = skip[spot, :] + jnp.dot(g[spot, :], ws[...], preferred_element_type=F32)
        a = jnp.maximum(v, 0.0).astype(BF16)
        m = jnp.maximum(jnp.dot(a, w1[...], preferred_element_type=F32) + c1[...], 0.0).astype(BF16)
        y[spot, :] = jnp.dot(m, w2[...], preferred_element_type=F32) + c2[...]
        copies.append(pltpu.make_async_copy(y.at[spot], y_hbm.at[spot], y_sem.at[tile]))
        if tile % 2:
            for c in copies[-2:]:
                c.start()
    h_copy.wait()
    for c in copies:
        c.wait()


def solution(mesh):
    n = mesh.shape["sp"]
    row_spec = P(("ens", "sp"), None)

    def local_stack(x_seq, w_past, w_now, b_conv, w_res, w_skip, w_out1, b_out1, w_out2, b_out2):
        stacks, cycle, res, _ = w_past.shape
        gate = b_conv.shape[-1] // 2
        skip_ch = w_skip.shape[-1]
        classes = w_out2.shape[-1]
        rows = x_seq.shape[0]
        layers = stacks * cycle
        tiles = rows // TILE
        args = (x_seq, w_past, w_now, b_conv, w_res, w_skip, w_out1, b_out1.reshape(1, -1), w_out2,
                b_out2.reshape(1, -1))
        args = [pltpu.with_memory_space_constraint(a, pltpu.HBM) for a in args]
        vmem = pl.BlockSpec(memory_space=pltpu.VMEM)
        anywhere = pl.BlockSpec(memory_space=pl.ANY)
        parts = pl.pallas_call(
            functools.partial(kernel, n, stacks, cycle),
            out_shape=(jax.ShapeDtypeStruct((rows, res), BF16),
                       jax.ShapeDtypeStruct((rows, skip_ch), F32),
                       jax.ShapeDtypeStruct((rows, gate), BF16),
                       jax.ShapeDtypeStruct((gate, skip_ch), BF16),
                       jax.ShapeDtypeStruct(w_out1.shape, BF16),
                       jax.ShapeDtypeStruct((1, skip_ch), F32),
                       jax.ShapeDtypeStruct(w_out2.shape, BF16),
                       jax.ShapeDtypeStruct((1, classes), F32)),
            in_specs=[anywhere] * 10,
            out_specs=(vmem,) * 8,
            scratch_shapes=[
                pltpu.VMEM((PAD + rows, res), BF16),
                pltpu.VMEM((layers - 1, rows, gate), BF16),
                pltpu.VMEM((layers, 2 * res, 2 * gate), BF16),
                pltpu.VMEM((layers,) + w_res.shape[2:], BF16),
                pltpu.VMEM((layers,) + w_skip.shape[2:], BF16),
                pltpu.VMEM(b_conv.shape, F32),
                pltpu.VMEM((layers + 1, PAD, res), BF16),
                pltpu.VMEM((layers, PAD, res), BF16),
                pltpu.SemaphoreType.DMA((tiles,)),
                pltpu.SemaphoreType.DMA((len(group_bounds(layers, cycle)),)),
                pltpu.SemaphoreType.DMA((6,)),
                pltpu.SemaphoreType.DMA((layers,)),
                pltpu.SemaphoreType.DMA((layers,)),
            ],
            compiler_params=pltpu.CompilerParams(
                collective_id=0, has_side_effects=True, vmem_limit_bytes=48 * 1024 * 1024),
            name="stack",
        )(*args)
        return pl.pallas_call(
            head,
            out_shape=(jax.ShapeDtypeStruct((rows, classes), F32), jax.ShapeDtypeStruct((rows, res), BF16)),
            in_specs=[vmem] * 8,
            out_specs=(anywhere, anywhere),
            scratch_shapes=[pltpu.VMEM((rows, classes), F32), pltpu.SemaphoreType.DMA,
                            pltpu.SemaphoreType.DMA((tiles,))],
            compiler_params=pltpu.CompilerParams(vmem_limit_bytes=16 * 1024 * 1024),
            name="head",
        )(*parts)

    return jax.shard_map(
        local_stack,
        mesh=mesh,
        in_specs=(row_spec, P(), P(), P(), P(), P(), P(), P(), P(), P()),
        out_specs=(row_spec, row_spec),
        check_vma=False,
    )
```
